32 devices in a mesh: row: 8 (over z, y), col: 4 (over x, core).
Axes of the slice: x: 2, y: 2, z: 4, core: 2. Of those that a mesh axis runs over, the one named last changes fastest.
Arguments:
- embeddings: float32 [32768, 2048], P('row', 'col'), may hold values from -2.5 to 2.5
- selected: int32 [512], replicated, may hold values from 0 to 32767, as said below
Outputs:
- sample_share: float32 [32768], P(('row', 'col'))
- log_gain: float32 [32768], P(('row', 'col'))
- logdet_mean: float32 [], replicated
The draws below stay inside these ranges and needn't reach their ends.
Inputs may be any that keep to these rules, and one draw needn't show every extreme that they name: `selected`: 512 distinct item indices.
All inputs are finite; a program needn't handle non-finite values.
Results may differ from the reference program's by a relative error of at most 0.0003.
Values sent between devices are 32-bit elements; how exact they have to be, the bound alone decides.
No kernel may reach another device: no remote copies, remote signals or barrier semaphores. Data moves between devices by JAX's collectives and lax.ppermute only.
A program may use at most 64 MiB of HBM per device.

```python
import math
import jax
import jax.numpy as jnp
from jax import lax

W = 2048
K = 512
CAND = 32768


def draw_embeddings(key, part):
    base_key = jax.random.fold_in(key, 11)
    key_entries, key_scale = jax.random.split(base_key, 2)
    position = jnp.arange(CAND, dtype=jnp.float32) / CAND
    entries = jax.random.normal(key_entries, (CAND, W), jnp.float32)
    growth = math.sqrt(3.0) ** position
    row_scale = jnp.exp(jax.random.uniform(key_scale, (CAND,), jnp.float32, 0.0, math.log(10.0))) * growth
    values = entries * row_scale[:, None] / math.sqrt(W)
    return jnp.clip(values, -2.5, 2.5).astype(jnp.float32)


def draw_selected(key, part):
    ordering = jax.random.permutation(jax.random.fold_in(key, 23), CAND)
    return ordering[:K].astype(jnp.int32)


def setup_inputs(seed: int = 0) -> dict:
    splits = jax.random.split(jax.random.key(seed), 3)
    embeddings = draw_embeddings(jax.random.fold_in(splits[2], 71), 0)
    selected = draw_selected(jax.random.fold_in(splits[2], 71), 0)
    return {"embeddings": embeddings, "selected": selected}


def reference(embeddings, selected):
    chosen = jnp.take(embeddings, selected, axis=0)
    kernel = jnp.dot(chosen, chosen.T, precision=lax.Precision.HIGHEST) + jnp.eye(K, dtype=chosen.dtype)
    factor = jnp.linalg.cholesky(kernel)
    logdet_mean = 2.0 * jnp.sum(jnp.log(jnp.diagonal(factor))) / K
    whitened = jax.scipy.linalg.solve_triangular(factor, chosen, lower=True)
    coordinates = jnp.dot(embeddings, whitened.T, precision=lax.Precision.HIGHEST)
    gain = jnp.sum(embeddings * embeddings, axis=1) + 1.0 - jnp.sum(coordinates * coordinates, axis=1)
    sample_share = gain * (CAND / jnp.sum(gain))
    return (sample_share, jnp.log(gain), logdet_mean)
```

```python
import functools
import math
import jax
import jax.numpy as jnp
from jax import lax
from jax.experimental import pallas as pl
from jax.experimental.pallas import tpu as pltpu
from jax.sharding import PartitionSpec as P

BLOCK = 128
HI = lax.Precision.HIGHEST
GROUP = 32
NEAR = 4


def eliminate(group, first, top, aug):
    tiles = group // 8
    row = lax.broadcasted_iota(jnp.int32, (8, BLOCK), 0)
    full = (8, BLOCK)
    p = [top[8 * t:8 * t + 8] for t in range(tiles)]
    q = [aug[8 * t:8 * t + 8] for t in range(tiles)]
    b = [[jnp.broadcast_to(p[t][:, first + k:first + k + 1], full) for t in range(tiles)] for k in range(group)]
    pivots = [jnp.ones(full, jnp.float32) for _ in range(tiles)]
    for j in range(group):
        tj, sj = divmod(j, 8)
        take = lambda v: jnp.broadcast_to(v[sj:sj + 1, :], full)
        pivot = take(b[j][tj])
        pivots[tj] = jnp.where(row == sj, pivot, pivots[tj])
        if j == group - 1:
            break
        inverse = 1.0 / pivot
        scale = {}
        for t in range(tj, tiles):
            m = b[j][t] * inverse
            scale[t] = jnp.where(row > sj, m, 0.0) if t == tj else m
        ts = [t for t in range(tj, tiles) if not (t == tj and sj == 7)]
        for k in range(j + 1, group):
            r = take(b[k][tj])
            for t in ts:
                b[k][t] = b[k][t] - scale[t] * r
        rp, rq = take(p[tj]), take(q[tj])
        for t in ts:
            p[t] = p[t] - scale[t] * rp
            q[t] = q[t] - scale[t] * rq
    for t in range(tiles):
        s = lax.rsqrt(pivots[t])
        p[t] = p[t] * s
        q[t] = q[t] * s
    logs = sum(jnp.log(v) for v in pivots)
    return jnp.concatenate(p, 0), jnp.concatenate(q, 0), logs


def dot(a, b, contract):
    return lax.dot_general(a, b, ((contract[:1], contract[1:]), ((), ())), precision=HI,
                           preferred_element_type=jnp.float32)


def invert(n, w_ref, d_ref, log_ref):
    r = lax.broadcasted_iota(jnp.int32, (BLOCK, BLOCK), 0)
    c = lax.broadcasted_iota(jnp.int32, (BLOCK, BLOCK), 1)
    eye = (r == c).astype(jnp.float32)
    log_ref[...] = jnp.zeros_like(log_ref)

    def step(k, carry):
        rows = pl.ds(pl.multiple_of(k * BLOCK, BLOCK), BLOCK)
        d_ref[:, :BLOCK] = w_ref[rows, rows]
        d_ref[:, BLOCK:] = eye
        logs = jnp.zeros((8, BLOCK), jnp.float32)
        for lo in range(0, BLOCK, GROUP):
            hi = lo + GROUP
            p, q, part = eliminate(GROUP, lo, d_ref[lo:hi, :BLOCK], d_ref[lo:hi, BLOCK:])
            logs = logs + part
            d_ref[lo:hi, BLOCK:] = q
            if hi < BLOCK:
                change = dot(p, jnp.concatenate([p, q], 1), (0, 0))
                d_ref[hi:, :] = d_ref[hi:, :] - change[hi:]
        log_ref[...] += logs
        window = pl.ds(pl.multiple_of((k + 1) * BLOCK, BLOCK), n)
        x = dot(d_ref[:, BLOCK:], w_ref[rows, window], (1, 0))
        w_ref[rows, window] = x

        def below(i, carry):
            to = pl.ds(pl.multiple_of(i * BLOCK, BLOCK), BLOCK)
            w_ref[to, window] -= dot(w_ref[rows, to], x, (0, 0))
            return carry

        return lax.fori_loop(k + 1, n // BLOCK, below, carry)

    lax.fori_loop(0, n // BLOCK, step, 0)


def identity(n):
    r = lax.broadcasted_iota(jnp.int32, (n, n), 0)
    c = lax.broadcasted_iota(jnp.int32, (n, n), 1)
    return (r == c).astype(jnp.float32)


def pairs(blocks):
    every = [(i, j) for i in range(blocks) for j in range(i, blocks)]
    return every[:len(every) // 2], every[len(every) // 2:]


def split(v, parts=2):
    out = []
    for _ in range(parts):
        out.append(v.astype(jnp.bfloat16))
        v = v - out[-1].astype(jnp.float32)
    return out


def product(a, b, contract):
    n = len(a)
    mul = lambda u, v: lax.dot_general(u, v, ((contract[:1], contract[1:]), ((), ())), preferred_element_type=jnp.float32)
    terms = [mul(a[i], b[k - i]) for k in reversed(range(n)) for i in range(k + 1)]
    return sum(terms[1:], terms[0])


def gram_kernel(core_ref, near_ref, rest_ref, near_other_ref, rest_other_ref, out_ref, *a_refs):
    near, width = near_ref.shape
    for rows, own, other in ((slice(0, near), near_ref, near_other_ref), (slice(near, None), rest_ref, rest_other_ref)):
        for a, u, v in zip(a_refs, split(own[...], 3), split(other[...], 3)):
            a[rows, :width], a[rows, width:] = u, v
    for t, (one, two) in enumerate(zip(*pairs(a_refs[0].shape[0] // BLOCK))):
        i, j = (pl.ds(pl.multiple_of(jnp.where(core_ref[0] == 0, u, v) * BLOCK, BLOCK), BLOCK) for u, v in zip(one, two))
        out_ref[t * BLOCK:(t + 1) * BLOCK, :] = product([a[i, :] for a in a_refs], [a[j, :] for a in a_refs], (1, 1))


def factor_kernel(core_ref, mine_ref, got_ref, inv_ref, log_ref, w_ref, d_ref):
    n = inv_ref.shape[0]
    w_ref[:, n:] = identity(n)
    w_ref[:, :n] = w_ref[:, n:]
    mine = core_ref[0]

    def place(which, ref):
        for t, (i, j) in enumerate(pairs(n // BLOCK)[which]):
            at = slice(i * BLOCK, (i + 1) * BLOCK), slice(j * BLOCK, (j + 1) * BLOCK)
            w_ref[at] = w_ref[at] + ref[t * BLOCK:(t + 1) * BLOCK, :]

    for which in range(2):
        pl.when(mine == which)(functools.partial(place, which, mine_ref))
        pl.when(mine != which)(functools.partial(place, which, got_ref))
    invert(n, w_ref, d_ref, log_ref)
    inv_ref[...] = w_ref[:, n:]


def score_kernel(at_ref, own_ref, other_ref, *refs):
    out_ref, pieces = refs[-1], refs[:-1]
    tile = jnp.concatenate([own_ref[...], other_ref[...]], 1)
    parts = split(tile)
    lo = 0
    for own, other in zip(pieces[::2], pieces[1::2]):
        n = own.shape[0]
        piece = jnp.concatenate([own[...], other[...]], 1)
        if n % BLOCK:
            piece = jnp.concatenate([piece, jnp.zeros((-n % BLOCK, piece.shape[1]), jnp.float32)], 0)
        out_ref[lo:lo + n, :] = jnp.transpose(product(parts, split(piece), (1, 1)))[:n]
        lo += n
    if lo < out_ref.shape[0]:
        squares = jnp.sum(tile * tile, 1, keepdims=True)
        out_ref[lo:, :] = jnp.transpose(jnp.broadcast_to(squares, (squares.shape[0], BLOCK)))[:out_ref.shape[0] - lo]


def score(which, block, embeddings, other_embeddings, norms, *pieces):
    tile = min(512, block)
    steps = block // tile
    items = sum(p.shape[0] for p in pieces[::2]) + (8 if norms else 0)
    width = embeddings.shape[1]
    candidates = pl.BlockSpec((tile, width), lambda i, at: (at[0] * steps + i, 0))
    return pl.pallas_call(
        score_kernel,
        out_shape=f32(items, block),
        grid_spec=pltpu.PrefetchScalarGridSpec(
            num_scalar_prefetch=1,
            grid=(steps,),
            in_specs=[candidates] * 2 + [pl.BlockSpec(p.shape, lambda i, at: (0, 0)) for p in pieces],
            out_specs=pl.BlockSpec((items, tile), lambda i, at: (0, i)),
        ),
        cost_estimate=pl.CostEstimate(flops=4 * items * block * width, bytes_accessed=8 * block * width, transcendentals=0),
    )(which.astype(jnp.int32)[None], embeddings, other_embeddings, *pieces)


def gain_kernel(inv_ref, log_ref, home_ref, near_ref, rest_ref, gain_ref, log_gain_ref, total_ref, *s_refs):
    n, near = inv_ref.shape[0], near_ref.shape[0] - 8
    for rows, got in ((slice(0, near), near_ref), (slice(near, n), rest_ref)):
        for s, v in zip(s_refs, split(home_ref[rows, :] + got[:rows.stop - rows.start, :])):
            s[rows, :] = v
    gain = home_ref[n:n + 1, :] + near_ref[near:near + 1, :] + 1.0
    for lo in range(0, n, BLOCK):
        hi = lo + BLOCK
        along = product(split(inv_ref[lo:hi, :hi]), [s[:hi, :] for s in s_refs], (1, 0))
        gain = gain - jnp.sum(along * along, 0, keepdims=True)
    gain_ref[...] = gain
    log_gain_ref[...] = jnp.log(gain)
    lane = lax.broadcasted_iota(jnp.int32, total_ref.shape, 1)
    logdet = jnp.sum(log_ref[...], 0, keepdims=True)[:, :1] / n
    total_ref[...] = jnp.where(lane == 0, jnp.sum(gain, 1, keepdims=True), logdet)


def share_kernel(count, sums_ref, gain_ref, out_ref, logdet_ref):
    total = jnp.sum(sums_ref[...], 0, keepdims=True)
    out_ref[...] = gain_ref[...] * (count / total[:, :1])
    logdet_ref[...] = sums_ref[:1, 1:2]


def pick_kernel(sel_ref, base_ref, table_ref, out_ref, at_ref, sem):
    slots, rows = out_ref.shape[0], table_ref.shape[0]
    base = base_ref[0]
    step = 16

    def scan(i, count):
        offsets = [sel_ref[i * step + j] - base for j in range(step)]
        inside = [((o >= 0) & (o < rows)).astype(jnp.int32) for o in offsets]
        for o, yes in zip(offsets, inside):
            at_ref[count] = o
            count = count + yes
        return count

    count = lax.fori_loop(0, sel_ref.shape[0] // step, scan, 0)

    def fill(k, carry):
        at_ref[k] = 0
        return carry

    lax.fori_loop(jnp.minimum(count, slots), slots, fill, 0)

    def start(i, carry):
        at = [at_ref[i * 8 + j] for j in range(8)]
        for j in range(8):
            pltpu.make_async_copy(table_ref.at[pl.ds(at[j], 1)], out_ref.at[pl.ds(i * 8 + j, 1)], sem).start()
        return carry

    lax.fori_loop(0, slots // 8, start, 0)
    pltpu.make_async_copy(out_ref, out_ref, sem).wait()


def join_kernel(first, even_ref, source_ref, slow_ref, *refs):
    blocks, out_ref, all_ref = refs[:-2], refs[-2], refs[-1]
    size, n = blocks[0].shape[0], out_ref.shape[0]

    @pl.when(even_ref[0] == 1)
    def _():
        for d, block in enumerate(blocks):
            all_ref[d * size:(d + 1) * size, :] = block[...]

        def copy(i, carry):
            at = [source_ref[i * 8 + j] for j in range(8)]
            out_ref[pl.ds(pl.multiple_of(i * 8, 8), 8), :] = jnp.concatenate([all_ref[pl.ds(a, 1), :] for a in at], 0)
            return carry

        lax.fori_loop(0, n // 8, copy, 0)

    @pl.when(even_ref[0] == 0)
    def _():
        pltpu.sync_copy(slow_ref.at[first:first + n], out_ref)


SMEM, VMEM, ANY = (pl.BlockSpec(memory_space=s) for s in (pltpu.SMEM, pltpu.VMEM, pl.ANY))


def f32(*shape):
    return jax.ShapeDtypeStruct(shape, jnp.float32)


def call(kernel, outs, specs, scratch, flops, *args):
    return pl.pallas_call(
        kernel,
        out_shape=outs,
        in_specs=specs,
        out_specs=(VMEM,) * len(outs) if isinstance(outs, tuple) else VMEM,
        scratch_shapes=scratch,
        cost_estimate=pl.CostEstimate(flops=flops, bytes_accessed=10 ** 6, transcendentals=0),
    )(*args)


def partner(size, distance):
    return [(i, i ^ distance) for i in range(size)]


def tie(value, *after):
    return lax.optimization_barrier((value,) + after)[0]


def any_split(embeddings, offsets):
    n = lax.axis_size("row")
    inside = (offsets >= 0) & (offsets < embeddings.shape[0])
    rows = jnp.take(embeddings, jnp.clip(offsets, 0, embeddings.shape[0] - 1), axis=0)
    rows = jnp.where(inside[:, None], rows, 0.0).reshape(n, -1, embeddings.shape[1])
    share = jnp.sum(lax.all_to_all(rows, "row", 0, 0), 0)
    out = lax.all_to_all(jnp.broadcast_to(share[None], (n,) + share.shape), "row", 0, 0)
    return out.reshape(-1, embeddings.shape[1])


def steps(embeddings, selected):
    rows_here, width = embeddings.shape
    picks = selected.shape[0]
    row_size, col_size = lax.axis_size("row"), lax.axis_size("col")
    row, col = lax.axis_index("row"), lax.axis_index("col")
    core, half = col % 2, col // 2
    block = rows_here // col_size
    to_core = lambda v: lax.ppermute(v, "col", partner(col_size, 1))
    to_chip = lambda v: lax.ppermute(v, "col", partner(col_size, 2))
    to_row = lambda v, s: lax.ppermute(v, "row", partner(row_size, s))
    which_core = core.astype(jnp.int32)[None]

    spread = lambda share: 4.25 * math.sqrt(picks * share * (1 - share))
    slots = min(picks, math.ceil((picks / row_size + spread(1 / row_size)) / 8) * 8)
    near_rows = max(8, int((picks * NEAR / row_size - spread(NEAR / row_size)) / 8) * 8)
    rest_rows = picks - near_rows

    other_embeddings = to_core(embeddings)

    rows = pl.pallas_call(
        pick_kernel,
        out_shape=f32(slots, width),
        in_specs=[SMEM, SMEM, ANY],
        out_specs=VMEM,
        scratch_shapes=[pltpu.SMEM((picks + 8,), jnp.int32), pltpu.SemaphoreType.DMA],
    )(selected, (row * rows_here)[None], embeddings)
    far = [to_row(rows, s) for s in range(NEAR, row_size, NEAR)]
    around = [rows] + [to_row(rows, s) for s in range(1, NEAR)]
    all_far = jnp.concatenate(far, 0)
    beyond = [all_far] + [to_row(all_far, s) for s in range(1, NEAR)]
    beyond = [v[m * slots:(m + 1) * slots] for m in range(len(far)) for v in beyond]

    picked = tie(selected, rows)
    shard = picked // rows_here
    number = jnp.arange(picks)
    before = number[None, :] < number[:, None]
    count = lambda mask: jnp.sum(mask, 1, dtype=jnp.int32)
    rank = count((shard[:, None] == shard[None, :]) & before)
    mine = shard // NEAR == row // NEAR
    place = count(mine[None, :] & (shard[None, :] < shard[:, None])) + rank
    is_near = mine & (place < near_rows)
    place = jnp.where(is_near, place, near_rows + count(before & ~is_near[None, :]))
    found = (shard ^ row) * slots + rank
    source = jnp.sum(jnp.where(place[None, :] == number[:, None], found[None, :], 0), 1)
    source = jnp.clip(source, 0, row_size * slots - 1)
    shards = jnp.arange(row_size)
    counts = count(shard[None, :] == shards[:, None])
    groups = count(shard[None, :] // NEAR == shards[:, None] // NEAR)
    even = jnp.all((counts <= slots) & (groups >= near_rows))
    slow = lax.cond(even, lambda v: jnp.zeros((picks, width), jnp.float32),
                    lambda v: any_split(embeddings, v - row * rows_here), picked)
    even = even.astype(jnp.int32)[None]

    def join(first, n, blocks):
        return call(functools.partial(join_kernel, first), f32(n, width), [SMEM, SMEM, ANY] + [VMEM] * len(blocks),
                    [pltpu.VMEM((len(blocks) * slots, width), jnp.float32)], 10 ** 8,
                    even, source[first:first + n], slow, *blocks)

    away, home = 2 * (1 - half) + core, 2 * half + core
    near = join(0, near_rows, around)
    near_other = to_core(near)
    score_near = score(away, block, embeddings, other_embeddings, True, near, near_other)
    got_near = to_chip(score_near)

    rest = join(near_rows, rest_rows, [tie(v, score_near) for v in around] + beyond)
    rest_other = to_core(rest)
    half_pairs = len(pairs(picks // BLOCK)[0]) * BLOCK
    gram = call(gram_kernel, f32(half_pairs, BLOCK), [SMEM] + [VMEM] * 4, [pltpu.VMEM((picks, 2 * width), jnp.bfloat16)] * 3,
                4 * 10 ** 8, which_core, near, rest, near_other, rest_other)
    gram_got = to_chip(gram)
    rest_t, rest_other_t, _ = lax.optimization_barrier((rest, rest_other, gram))
    score_rest = score(away, block, embeddings, other_embeddings, False, rest_t, rest_other_t)
    got_rest = to_chip(score_rest)
    near_t, near_other_t, _ = lax.optimization_barrier((near, near_other, score_rest))
    score_home = score(home, block, embeddings, other_embeddings, True, near_t, near_other_t, rest_t, rest_other_t)

    gram = tie(gram + gram_got, score_home)
    inverse, logs = call(factor_kernel, (f32(picks, picks), f32(8, BLOCK)), [SMEM] + [VMEM] * 2,
                         [pltpu.VMEM((picks, 2 * picks), jnp.float32), pltpu.VMEM((BLOCK, 2 * BLOCK), jnp.float32)],
                         4 * 10 ** 9, which_core, gram, to_core(gram))

    devices = row_size * col_size
    gain, log_gain, total = call(gain_kernel, (f32(1, block), f32(1, block), f32(devices, BLOCK)), [VMEM] * 5,
                                 [pltpu.VMEM((picks, block), jnp.bfloat16)] * 2, 10 ** 8,
                                 inverse, logs, score_home, got_near, got_rest)
    totals = lax.all_to_all(total.reshape(devices, 1, BLOCK), ("row", "col"), 0, 0).reshape(devices, BLOCK)
    share, logdet = call(functools.partial(share_kernel, rows_here * row_size), (f32(1, block), f32(1, 1)), [VMEM] * 2, [],
                         10 ** 7, totals, gain)
    return (share.reshape(block), log_gain.reshape(block), logdet.reshape(()))


def solution(mesh):
    return jax.shard_map(
        steps,
        mesh=mesh,
        in_specs=(P("row", "col"), P()),
        out_specs=(P(("row", "col")), P(("row", "col")), P()),
        check_vma=False,
    )
```

```python
import functools
import math
import jax
import jax.numpy as jnp
from jax import lax
from jax.experimental import pallas as pl
from jax.experimental.pallas import tpu as pltpu
from jax.sharding import PartitionSpec as P

BLOCK = 128
HI = lax.Precision.HIGHEST
GROUP = 32
NEAR = 4


def eliminate(group, first, top, aug):
    tiles = group // 8
    row = lax.broadcasted_iota(jnp.int32, (8, BLOCK), 0)
    full = (8, BLOCK)
    p = [top[8 * t:8 * t + 8] for t in range(tiles)]
    q = [aug[8 * t:8 * t + 8] for t in range(tiles)]
    b = [[jnp.broadcast_to(p[t][:, first + k:first + k + 1], full) for t in range(tiles)] for k in range(group)]
    pivots = [jnp.ones(full, jnp.float32) for _ in range(tiles)]
    for j in range(group):
        tj, sj = divmod(j, 8)
        take = lambda v: jnp.broadcast_to(v[sj:sj + 1, :], full)
        pivot = take(b[j][tj])
        pivots[tj] = jnp.where(row == sj, pivot, pivots[tj])
        if j == group - 1:
            break
        inverse = 1.0 / pivot
        scale = {}
        for t in range(tj, tiles):
            m = b[j][t] * inverse
            scale[t] = jnp.where(row > sj, m, 0.0) if t == tj else m
        ts = [t for t in range(tj, tiles) if not (t == tj and sj == 7)]
        for k in range(j + 1, group):
            r = take(b[k][tj])
            for t in ts:
                b[k][t] = b[k][t] - scale[t] * r
        rp, rq = take(p[tj]), take(q[tj])
        for t in ts:
            p[t] = p[t] - scale[t] * rp
            q[t] = q[t] - scale[t] * rq
    for t in range(tiles):
        s = lax.rsqrt(pivots[t])
        p[t] = p[t] * s
        q[t] = q[t] * s
    logs = sum(jnp.log(v) for v in pivots)
    return jnp.concatenate(p, 0), jnp.concatenate(q, 0), logs


def dot(a, b, contract):
    return lax.dot_general(a, b, ((contract[:1], contract[1:]), ((), ())), precision=HI,
                           preferred_element_type=jnp.float32)


def invert(n, w_ref, d_ref, log_ref):
    r = lax.broadcasted_iota(jnp.int32, (BLOCK, BLOCK), 0)
    c = lax.broadcasted_iota(jnp.int32, (BLOCK, BLOCK), 1)
    eye = (r == c).astype(jnp.float32)
    log_ref[...] = jnp.zeros_like(log_ref)

    def step(k, carry):
        rows = pl.ds(pl.multiple_of(k * BLOCK, BLOCK), BLOCK)
        d_ref[:, :BLOCK] = w_ref[rows, rows]
        d_ref[:, BLOCK:] = eye
        logs = jnp.zeros((8, BLOCK), jnp.float32)
        for lo in range(0, BLOCK, GROUP):
            hi = lo + GROUP
            p, q, part = eliminate(GROUP, lo, d_ref[lo:hi, :BLOCK], d_ref[lo:hi, BLOCK:])
            logs = logs + part
            d_ref[lo:hi, BLOCK:] = q
            if hi < BLOCK:
                change = dot(p, jnp.concatenate([p, q], 1), (0, 0))
                d_ref[hi:, :] = d_ref[hi:, :] - change[hi:]
        log_ref[...] += logs
        window = pl.ds(pl.multiple_of((k + 1) * BLOCK, BLOCK), n)
        x = dot(d_ref[:, BLOCK:], w_ref[rows, window], (1, 0))
        w_ref[rows, window] = x

        def below(i, carry):
            to = pl.ds(pl.multiple_of(i * BLOCK, BLOCK), BLOCK)
            w_ref[to, window] -= dot(w_ref[rows, to], x, (0, 0))
            return carry

        return lax.fori_loop(k + 1, n // BLOCK, below, carry)

    lax.fori_loop(0, n // BLOCK, step, 0)


def identity(n):
    r = lax.broadcasted_iota(jnp.int32, (n, n), 0)
    c = lax.broadcasted_iota(jnp.int32, (n, n), 1)
    return (r == c).astype(jnp.float32)


def pairs(blocks):
    every = [(i, j) for i in range(blocks) for j in range(i, blocks)]
    return every[:len(every) // 2], every[len(every) // 2:]


def split(v, parts=2):
    out = []
    for _ in range(parts):
        out.append(v.astype(jnp.bfloat16))
        v = v - out[-1].astype(jnp.float32)
    return out


def product(a, b, contract):
    n = len(a)
    mul = lambda u, v: lax.dot_general(u, v, ((contract[:1], contract[1:]), ((), ())), preferred_element_type=jnp.float32)
    terms = [mul(a[i], b[k - i]) for k in reversed(range(n)) for i in range(k + 1)]
    return sum(terms[1:], terms[0])


def gram_kernel(core_ref, near_ref, rest_ref, near_other_ref, rest_other_ref, out_ref, *a_refs):
    near, width = near_ref.shape
    for rows, own, other in ((slice(0, near), near_ref, near_other_ref), (slice(near, None), rest_ref, rest_other_ref)):
        for a, u, v in zip(a_refs, split(own[...], 3), split(other[...], 3)):
            a[rows, :width], a[rows, width:] = u, v
    for t, (one, two) in enumerate(zip(*pairs(a_refs[0].shape[0] // BLOCK))):
        i, j = (pl.ds(pl.multiple_of(jnp.where(core_ref[0] == 0, u, v) * BLOCK, BLOCK), BLOCK) for u, v in zip(one, two))
        out_ref[t * BLOCK:(t + 1) * BLOCK, :] = product([a[i, :] for a in a_refs], [a[j, :] for a in a_refs], (1, 1))


def factor_kernel(core_ref, mine_ref, got_ref, inv_ref, log_ref, w_ref, d_ref):
    n = inv_ref.shape[0]
    w_ref[:, n:] = identity(n)
    w_ref[:, :n] = w_ref[:, n:]
    mine = core_ref[0]

    def place(which, ref):
        for t, (i, j) in enumerate(pairs(n // BLOCK)[which]):
            at = slice(i * BLOCK, (i + 1) * BLOCK), slice(j * BLOCK, (j + 1) * BLOCK)
            w_ref[at] = w_ref[at] + ref[t * BLOCK:(t + 1) * BLOCK, :]

    for which in range(2):
        pl.when(mine == which)(functools.partial(place, which, mine_ref))
        pl.when(mine != which)(functools.partial(place, which, got_ref))
    invert(n, w_ref, d_ref, log_ref)
    inv_ref[...] = w_ref[:, n:]


def prepare_kernel(at_ref, own_ref, other_ref, high_ref, low_ref, norm_ref, tile_ref, sems):
    size, width = tile_ref.shape[1], own_ref.shape[1]
    count = high_ref.shape[0] // size

    def copies(t):
        rows = pl.ds(pl.multiple_of(at_ref[0] + t * size, size), size)
        return [pltpu.make_async_copy(ref.at[rows], tile_ref.at[t % 2, :, side * width:(side + 1) * width], sems.at[t % 2, side])
                for side, ref in enumerate((own_ref, other_ref))]

    def start(t):
        for copy in copies(t):
            copy.start()

    start(0)
    for t in range(count):
        if t + 1 < count:
            start(t + 1)
        for copy in copies(t):
            copy.wait()
        tile = tile_ref[t % 2]
        rows = slice(t * size, (t + 1) * size)
        high_ref[rows, :], low_ref[rows, :] = split(tile)
        squares = jnp.sum(tile * tile, 1, keepdims=True)
        norm_ref[:, rows] = jnp.transpose(jnp.broadcast_to(squares, (size, BLOCK)))[:8]


def score_kernel(high_ref, low_ref, *refs):
    *pieces, out_ref = refs
    norms = [pieces.pop()] if len(pieces) % 2 else []
    size = min(512, high_ref.shape[0])
    selected = []
    for own, other in zip(pieces[::2], pieces[1::2]):
        piece = jnp.concatenate([own[...], other[...]], 1)
        if own.shape[0] % BLOCK:
            piece = jnp.concatenate([piece, jnp.zeros((-own.shape[0] % BLOCK, piece.shape[1]), jnp.float32)], 0)
        selected.append((own.shape[0], split(piece)))
    for t in range(high_ref.shape[0] // size):
        rows = slice(t * size, (t + 1) * size)
        parts = [high_ref[rows, :], low_ref[rows, :]]
        lo = 0
        for n, piece in selected:
            out_ref[lo:lo + n, rows] = jnp.transpose(product(parts, piece, (1, 1)))[:n]
            lo += n
    for norm in norms:
        out_ref[lo:, :] = norm[...]


def prepare(which, block, embeddings, other_embeddings):
    tile, width = min(256, block), embeddings.shape[1]
    part = jax.ShapeDtypeStruct((block, 2 * width), jnp.bfloat16)
    return call(prepare_kernel, (part, part, f32(8, block)), [SMEM, ANY, ANY],
                [pltpu.VMEM((2, tile, 2 * width), jnp.float32), pltpu.SemaphoreType.DMA((2, 2))],
                10 ** 9, (which * block).astype(jnp.int32)[None], embeddings, other_embeddings)


def score(prepared, *pieces):
    block, items = prepared[0].shape[0], sum(p.shape[0] for p in pieces[::2]) + (8 if len(prepared) > 2 else 0)
    return call(score_kernel, f32(items, block), [VMEM] * (len(pieces) + len(prepared)), [], 10 ** 9,
                *prepared[:2], *pieces, *prepared[2:])


def gain_kernel(inv_ref, log_ref, norm_ref, home_ref, near_ref, rest_ref, gain_ref, log_gain_ref, total_ref, *s_refs):
    n, near = inv_ref.shape[0], near_ref.shape[0] - 8
    for rows, got in ((slice(0, near), near_ref), (slice(near, n), rest_ref)):
        for s, v in zip(s_refs, split(home_ref[rows, :] + got[:rows.stop - rows.start, :])):
            s[rows, :] = v
    gain = norm_ref[:1, :] + near_ref[near:near + 1, :] + 1.0
    for lo in range(0, n, BLOCK):
        hi = lo + BLOCK
        along = product(split(inv_ref[lo:hi, :hi]), [s[:hi, :] for s in s_refs], (1, 0))
        gain = gain - jnp.sum(along * along, 0, keepdims=True)
    gain_ref[...] = gain
    log_gain_ref[...] = jnp.log(gain)
    lane = lax.broadcasted_iota(jnp.int32, total_ref.shape, 1)
    logdet = jnp.sum(log_ref[...], 0, keepdims=True)[:, :1] / n
    total_ref[...] = jnp.where(lane == 0, jnp.sum(gain, 1, keepdims=True), logdet)


def share_kernel(count, sums_ref, gain_ref, out_ref, logdet_ref):
    total = jnp.sum(sums_ref[...], 0, keepdims=True)
    out_ref[...] = gain_ref[...] * (count / total[:, :1])
    logdet_ref[...] = sums_ref[:1, 1:2]


def pick_kernel(sel_ref, base_ref, table_ref, out_ref, at_ref, sem):
    slots, rows = out_ref.shape[0], table_ref.shape[0]
    base = base_ref[0]
    step = 16

    def scan(i, count):
        offsets = [sel_ref[i * step + j] - base for j in range(step)]
        inside = [((o >= 0) & (o < rows)).astype(jnp.int32) for o in offsets]
        for o, yes in zip(offsets, inside):
            at_ref[count] = o
            count = count + yes
        return count

    count = lax.fori_loop(0, sel_ref.shape[0] // step, scan, 0)

    def fill(k, carry):
        at_ref[k] = 0
        return carry

    lax.fori_loop(jnp.minimum(count, slots), slots, fill, 0)

    def start(i, carry):
        at = [at_ref[i * 8 + j] for j in range(8)]
        for j in range(8):
            pltpu.make_async_copy(table_ref.at[pl.ds(at[j], 1)], out_ref.at[pl.ds(i * 8 + j, 1)], sem).start()
        return carry

    lax.fori_loop(0, slots // 8, start, 0)
    pltpu.make_async_copy(out_ref, out_ref, sem).wait()


def join_kernel(first, even_ref, source_ref, slow_ref, *refs):
    blocks, out_ref, all_ref = refs[:-2], refs[-2], refs[-1]
    size, n = blocks[0].shape[0], out_ref.shape[0]

    @pl.when(even_ref[0] == 1)
    def _():
        for d, block in enumerate(blocks):
            all_ref[d * size:(d + 1) * size, :] = block[...]

        def copy(i, carry):
            at = [source_ref[first + i * 8 + j] for j in range(8)]
            out_ref[pl.ds(pl.multiple_of(i * 8, 8), 8), :] = jnp.concatenate([all_ref[pl.ds(a, 1), :] for a in at], 0)
            return carry

        lax.fori_loop(0, n // 8, copy, 0)

    @pl.when(even_ref[0] == 0)
    def _():
        pltpu.sync_copy(slow_ref.at[first:first + n], out_ref)


SMEM, VMEM, ANY = (pl.BlockSpec(memory_space=s) for s in (pltpu.SMEM, pltpu.VMEM, pl.ANY))


def f32(*shape):
    return jax.ShapeDtypeStruct(shape, jnp.float32)


GRANT = pltpu.CompilerParams(vmem_limit_bytes=20 * 2 ** 20)


def call(kernel, outs, specs, scratch, flops, *args):
    return pl.pallas_call(
        kernel,
        out_shape=outs,
        in_specs=specs,
        out_specs=(VMEM,) * len(outs) if isinstance(outs, tuple) else VMEM,
        scratch_shapes=scratch,
        cost_estimate=pl.CostEstimate(flops=flops, bytes_accessed=10 ** 6, transcendentals=0),
        compiler_params=GRANT,
    )(*args)


def partner(size, distance):
    return [(i, i ^ distance) for i in range(size)]


def tie(value, *after):
    return lax.optimization_barrier((value,) + after)[0]


def any_split(embeddings, offsets):
    n = lax.axis_size("row")
    inside = (offsets >= 0) & (offsets < embeddings.shape[0])
    rows = jnp.take(embeddings, jnp.clip(offsets, 0, embeddings.shape[0] - 1), axis=0)
    rows = jnp.where(inside[:, None], rows, 0.0).reshape(n, -1, embeddings.shape[1])
    share = jnp.sum(lax.all_to_all(rows, "row", 0, 0), 0)
    out = lax.all_to_all(jnp.broadcast_to(share[None], (n,) + share.shape), "row", 0, 0)
    return out.reshape(-1, embeddings.shape[1])


def steps(embeddings, selected):
    rows_here, width = embeddings.shape
    picks = selected.shape[0]
    row_size, col_size = lax.axis_size("row"), lax.axis_size("col")
    row, col = lax.axis_index("row"), lax.axis_index("col")
    core, half = col % 2, col // 2
    block = rows_here // col_size
    to_core = lambda v: lax.ppermute(v, "col", partner(col_size, 1))
    to_chip = lambda v: lax.ppermute(v, "col", partner(col_size, 2))
    to_row = lambda v, s: lax.ppermute(v, "row", partner(row_size, s))
    which_core = core.astype(jnp.int32)[None]

    spread = lambda share: 4.25 * math.sqrt(picks * share * (1 - share))
    slots = min(picks, math.ceil((picks / row_size + spread(1 / row_size)) / 8) * 8)
    near_rows = max(8, int((picks * NEAR / row_size - spread(NEAR / row_size)) / 8) * 8)
    rest_rows = picks - near_rows

    other_embeddings = to_core(embeddings)

    rows = pl.pallas_call(
        pick_kernel,
        out_shape=f32(slots, width),
        in_specs=[SMEM, SMEM, ANY],
        out_specs=VMEM,
        scratch_shapes=[pltpu.SMEM((picks + 8,), jnp.int32), pltpu.SemaphoreType.DMA],
        compiler_params=GRANT,
    )(selected, (row * rows_here)[None], embeddings)
    far = [to_row(rows, s) for s in range(NEAR, row_size, NEAR)]
    around = [rows] + [to_row(rows, s) for s in range(1, NEAR)]
    all_far = jnp.concatenate(far, 0)
    beyond = [all_far] + [to_row(all_far, s) for s in range(1, NEAR)]
    beyond = [v[m * slots:(m + 1) * slots] for m in range(len(far)) for v in beyond]

    picked = tie(selected, rows)
    shard = picked // rows_here
    number = jnp.arange(picks)
    before = number[None, :] < number[:, None]
    count = lambda mask: jnp.sum(mask, 1, dtype=jnp.int32)
    rank = count((shard[:, None] == shard[None, :]) & before)
    mine = shard // NEAR == row // NEAR
    place = count(mine[None, :] & (shard[None, :] < shard[:, None])) + rank
    is_near = mine & (place < near_rows)
    place = jnp.where(is_near, place, near_rows + count(before & ~is_near[None, :]))
    found = (shard ^ row) * slots + rank
    source = jnp.sum(jnp.where(place[None, :] == number[:, None], found[None, :], 0), 1)
    source = jnp.clip(source, 0, row_size * slots - 1)
    shards = jnp.arange(row_size)
    counts = count(shard[None, :] == shards[:, None])
    groups = count(shard[None, :] // NEAR == shards[:, None] // NEAR)
    even = jnp.all((counts <= slots) & (groups >= near_rows))
    slow = lax.cond(even, lambda v: jnp.zeros((picks, width), jnp.float32),
                    lambda v: any_split(embeddings, v - row * rows_here), picked)
    even = even.astype(jnp.int32)[None]

    def join(first, n, blocks):
        return call(functools.partial(join_kernel, first), f32(n, width), [SMEM, SMEM, ANY] + [VMEM] * len(blocks),
                    [pltpu.VMEM((len(blocks) * slots, width), jnp.float32)], 10 ** 8,
                    even, source, slow, *blocks)

    away = prepare(2 * (1 - half) + core, block, embeddings, other_embeddings)
    near = join(0, near_rows, around)
    near_other = to_core(near)
    score_near = score(away, near, near_other)
    got_near = to_chip(score_near)

    rest = join(near_rows, rest_rows, [tie(v, score_near) for v in around] + beyond)
    rest_other = to_core(rest)
    half_pairs = len(pairs(picks // BLOCK)[0]) * BLOCK
    gram = call(gram_kernel, f32(half_pairs, BLOCK), [SMEM] + [VMEM] * 4, [pltpu.VMEM((picks, 2 * width), jnp.bfloat16)] * 3,
                4 * 10 ** 8, which_core, near, rest, near_other, rest_other)
    gram_got = to_chip(gram)
    rest_t, rest_other_t, _ = lax.optimization_barrier((rest, rest_other, gram))
    score_rest = score(away[:2], rest_t, rest_other_t)
    got_rest = to_chip(score_rest)
    near_t, near_other_t, _ = lax.optimization_barrier((near, near_other, score_rest))
    home = prepare(2 * half + core, block, tie(embeddings, score_rest), other_embeddings)
    score_home = score(home[:2], near_t, near_other_t, rest_t, rest_other_t)

    gram = tie(gram + gram_got, score_home)
    inverse, logs = call(factor_kernel, (f32(picks, picks), f32(8, BLOCK)), [SMEM] + [VMEM] * 2,
                         [pltpu.VMEM((picks, 2 * picks), jnp.float32), pltpu.VMEM((BLOCK, 2 * BLOCK), jnp.float32)],
                         4 * 10 ** 9, which_core, gram, to_core(gram))

    devices = row_size * col_size
    gain, log_gain, total = call(gain_kernel, (f32(1, block), f32(1, block), f32(devices, BLOCK)), [VMEM] * 6,
                                 [pltpu.VMEM((picks, block), jnp.bfloat16)] * 2, 10 ** 8,
                                 inverse, logs, home[2], score_home, got_near, got_rest)
    totals = lax.all_to_all(total.reshape(devices, 1, BLOCK), ("row", "col"), 0, 0).reshape(devices, BLOCK)
    share, logdet = call(functools.partial(share_kernel, rows_here * row_size), (f32(1, block), f32(1, 1)), [VMEM] * 2, [],
                         10 ** 7, totals, gain)
    return (share.reshape(block), log_gain.reshape(block), logdet.reshape(()))


def solution(mesh):
    return jax.shard_map(
        steps,
        mesh=mesh,
        in_specs=(P("row", "col"), P()),
        out_specs=(P(("row", "col")), P(("row", "col")), P()),
        check_vma=False,
    )
```

```python
import functools
import math
import jax
import jax.numpy as jnp
from jax import lax
from jax.experimental import pallas as pl
from jax.experimental.pallas import tpu as pltpu
from jax.sharding import PartitionSpec as P

BLOCK = 128
HI = lax.Precision.HIGHEST
GROUP = 32
NEAR = 4


def eliminate(group, first, top, aug):
    tiles = group // 8
    row = lax.broadcasted_iota(jnp.int32, (8, BLOCK), 0)
    full = (8, BLOCK)
    p = [top[8 * t:8 * t + 8] for t in range(tiles)]
    q = [aug[8 * t:8 * t + 8] for t in range(tiles)]
    b = [[jnp.broadcast_to(p[t][:, first + k:first + k + 1], full) for t in range(tiles)] for k in range(group)]
    pivots = [jnp.ones(full, jnp.float32) for _ in range(tiles)]
    for j in range(group):
        tj, sj = divmod(j, 8)
        take = lambda v: jnp.broadcast_to(v[sj:sj + 1, :], full)
        pivot = take(b[j][tj])
        pivots[tj] = jnp.where(row == sj, pivot, pivots[tj])
        if j == group - 1:
            break
        inverse = 1.0 / pivot
        scale = {}
        for t in range(tj, tiles):
            m = b[j][t] * inverse
            scale[t] = jnp.where(row > sj, m, 0.0) if t == tj else m
        ts = [t for t in range(tj, tiles) if not (t == tj and sj == 7)]
        for k in range(j + 1, group):
            r = take(b[k][tj])
            for t in ts:
                b[k][t] = b[k][t] - scale[t] * r
        rp, rq = take(p[tj]), take(q[tj])
        for t in ts:
            p[t] = p[t] - scale[t] * rp
            q[t] = q[t] - scale[t] * rq
    for t in range(tiles):
        s = lax.rsqrt(pivots[t])
        p[t] = p[t] * s
        q[t] = q[t] * s
    logs = sum(jnp.log(v) for v in pivots)
    return jnp.concatenate(p, 0), jnp.concatenate(q, 0), logs


def dot(a, b, contract):
    return lax.dot_general(a, b, ((contract[:1], contract[1:]), ((), ())), precision=HI,
                           preferred_element_type=jnp.float32)


def invert(n, w_ref, d_ref, log_ref):
    r = lax.broadcasted_iota(jnp.int32, (BLOCK, BLOCK), 0)
    c = lax.broadcasted_iota(jnp.int32, (BLOCK, BLOCK), 1)
    eye = (r == c).astype(jnp.float32)
    log_ref[...] = jnp.zeros_like(log_ref)

    def step(k, carry):
        rows = pl.ds(pl.multiple_of(k * BLOCK, BLOCK), BLOCK)
        d_ref[:, :BLOCK] = w_ref[rows, rows]
        d_ref[:, BLOCK:] = eye
        logs = jnp.zeros((8, BLOCK), jnp.float32)
        for lo in range(0, BLOCK, GROUP):
            hi = lo + GROUP
            p, q, part = eliminate(GROUP, lo, d_ref[lo:hi, :BLOCK], d_ref[lo:hi, BLOCK:])
            logs = logs + part
            d_ref[lo:hi, BLOCK:] = q
            if hi < BLOCK:
                change = dot(p, jnp.concatenate([p, q], 1), (0, 0))
                d_ref[hi:, :] = d_ref[hi:, :] - change[hi:]
        log_ref[...] += logs
        window = pl.ds(pl.multiple_of((k + 1) * BLOCK, BLOCK), n)
        x = dot(d_ref[:, BLOCK:], w_ref[rows, window], (1, 0))
        w_ref[rows, window] = x

        def below(i, carry):
            to = pl.ds(pl.multiple_of(i * BLOCK, BLOCK), BLOCK)
            w_ref[to, window] -= dot(w_ref[rows, to], x, (0, 0))
            return carry

        return lax.fori_loop(k + 1, n // BLOCK, below, carry)

    lax.fori_loop(0, n // BLOCK, step, 0)


def identity(n):
    r = lax.broadcasted_iota(jnp.int32, (n, n), 0)
    c = lax.broadcasted_iota(jnp.int32, (n, n), 1)
    return (r == c).astype(jnp.float32)


def pairs(blocks):
    every = [(i, j) for i in range(blocks) for j in range(i, blocks)]
    return every[:len(every) // 2], every[len(every) // 2:]


def split(v, parts=2):
    out = []
    for _ in range(parts):
        out.append(v.astype(jnp.bfloat16))
        v = v - out[-1].astype(jnp.float32)
    return out


def product(a, b, contract):
    n = len(a)
    mul = lambda u, v: lax.dot_general(u, v, ((contract[:1], contract[1:]), ((), ())), preferred_element_type=jnp.float32)
    terms = [mul(a[i], b[k - i]) for k in reversed(range(n)) for i in range(k + 1)]
    return sum(terms[1:], terms[0])


def gram_kernel(core_ref, *refs):
    a_refs, out_ref, pieces = refs[-3:], refs[-4], refs[:-4]
    lo = 0
    for own, other in zip(pieces[::2], pieces[1::2]):
        n, width = own.shape
        for a, u, v in zip(a_refs, split(own[...], 3), split(other[...], 3)):
            a[lo:lo + n, :width], a[lo:lo + n, width:] = u, v
        lo += n
    for t, (one, two) in enumerate(zip(*pairs(lo // BLOCK))):
        i, j = (pl.ds(pl.multiple_of(jnp.where(core_ref[0] == 0, u, v) * BLOCK, BLOCK), BLOCK) for u, v in zip(one, two))
        out_ref[t * BLOCK:(t + 1) * BLOCK, :] = product([a[i, :] for a in a_refs], [a[j, :] for a in a_refs], (1, 1))


def factor_kernel(core_ref, mine_ref, got_ref, inv_ref, log_ref, w_ref, d_ref):
    n = inv_ref.shape[0]
    w_ref[:, n:] = identity(n)
    w_ref[:, :n] = w_ref[:, n:]
    mine = core_ref[0]

    def place(which, ref):
        for t, (i, j) in enumerate(pairs(n // BLOCK)[which]):
            at = slice(i * BLOCK, (i + 1) * BLOCK), slice(j * BLOCK, (j + 1) * BLOCK)
            w_ref[at] = w_ref[at] + ref[t * BLOCK:(t + 1) * BLOCK, :]

    for which in range(2):
        pl.when(mine == which)(functools.partial(place, which, mine_ref))
        pl.when(mine != which)(functools.partial(place, which, got_ref))
    invert(n, w_ref, d_ref, log_ref)
    inv_ref[...] = w_ref[:, n:]


def prepare_kernel(at_ref, own_ref, other_ref, high_ref, low_ref, norm_ref, tile_ref, sems):
    size, width = tile_ref.shape[1], own_ref.shape[1]
    count = high_ref.shape[0] // size

    def copies(t):
        rows = pl.ds(pl.multiple_of(at_ref[0] + t * size, size), size)
        return [pltpu.make_async_copy(ref.at[rows], tile_ref.at[t % 2, :, side * width:(side + 1) * width], sems.at[t % 2, side])
                for side, ref in enumerate((own_ref, other_ref))]

    def start(t):
        for copy in copies(t):
            copy.start()

    start(0)
    for t in range(count):
        if t + 1 < count:
            start(t + 1)
        for copy in copies(t):
            copy.wait()
        tile = tile_ref[t % 2]
        rows = slice(t * size, (t + 1) * size)
        high_ref[rows, :], low_ref[rows, :] = split(tile)
        squares = jnp.sum(tile * tile, 1, keepdims=True)
        norm_ref[:, rows] = jnp.transpose(jnp.broadcast_to(squares, (size, BLOCK)))[:8]


def score_kernel(high_ref, low_ref, *refs):
    *pieces, out_ref = refs
    norms = [pieces.pop()] if len(pieces) % 2 else []
    size = min(512, high_ref.shape[0])
    rows = [jnp.concatenate([own[...], other[...]], 1) for own, other in zip(pieces[::2], pieces[1::2])]
    items = sum(v.shape[0] for v in rows)
    if items % BLOCK:
        rows.append(jnp.zeros((-items % BLOCK, rows[0].shape[1]), jnp.float32))
    selected = split(jnp.concatenate(rows, 0))
    for t in range(high_ref.shape[0] // size):
        at = slice(t * size, (t + 1) * size)
        out_ref[:items, at] = jnp.transpose(product([high_ref[at, :], low_ref[at, :]], selected, (1, 1)))[:items]
    for norm in norms:
        out_ref[items:, :] = norm[...]


def prepare(which, block, embeddings, other_embeddings):
    tile, width = min(256, block), embeddings.shape[1]
    part = jax.ShapeDtypeStruct((block, 2 * width), jnp.bfloat16)
    return call(prepare_kernel, (part, part, f32(8, block)), [SMEM, ANY, ANY],
                [pltpu.VMEM((2, tile, 2 * width), jnp.float32), pltpu.SemaphoreType.DMA((2, 2))],
                10 ** 9, (which * block).astype(jnp.int32)[None], embeddings, other_embeddings)


def score(prepared, *pieces):
    block, items = prepared[0].shape[0], sum(p.shape[0] for p in pieces[::2]) + (8 if len(prepared) > 2 else 0)
    return call(score_kernel, f32(items, block), [VMEM] * (len(pieces) + len(prepared)), [], 10 ** 9,
                *prepared[:2], *pieces, *prepared[2:])


def gain_kernel(sizes, inv_ref, log_ref, norm_ref, home_ref, *refs):
    n, got_refs = inv_ref.shape[0], refs[:len(sizes)]
    gain_ref, log_gain_ref, total_ref, *s_refs = refs[len(sizes):]
    lo = 0
    for size, got in zip(sizes, got_refs):
        for s, v in zip(s_refs, split(home_ref[lo:lo + size, :] + got[:size, :])):
            s[lo:lo + size, :] = v
        lo += size
    gain = norm_ref[:1, :] + got_refs[0][sizes[0]:sizes[0] + 1, :] + 1.0
    for lo in range(0, n, BLOCK):
        hi = lo + BLOCK
        along = product(split(inv_ref[lo:hi, :hi]), [s[:hi, :] for s in s_refs], (1, 0))
        gain = gain - jnp.sum(along * along, 0, keepdims=True)
    gain_ref[...] = gain
    log_gain_ref[...] = jnp.log(gain)
    lane = lax.broadcasted_iota(jnp.int32, total_ref.shape, 1)
    logdet = jnp.sum(log_ref[...], 0, keepdims=True)[:, :1] / n
    total_ref[...] = jnp.where(lane == 0, jnp.sum(gain, 1, keepdims=True), logdet)


def share_kernel(count, sums_ref, gain_ref, out_ref, logdet_ref):
    total = jnp.sum(sums_ref[...], 0, keepdims=True)
    out_ref[...] = gain_ref[...] * (count / total[:, :1])
    logdet_ref[...] = sums_ref[:1, 1:2]


def pick_kernel(sel_ref, base_ref, table_ref, out_ref, at_ref, sem):
    slots, rows = out_ref.shape[0], table_ref.shape[0]
    base = base_ref[0]
    step = 16

    def scan(i, count):
        offsets = [sel_ref[i * step + j] - base for j in range(step)]
        inside = [((o >= 0) & (o < rows)).astype(jnp.int32) for o in offsets]
        for o, yes in zip(offsets, inside):
            at_ref[count] = o
            count = count + yes
        return count

    count = lax.fori_loop(0, sel_ref.shape[0] // step, scan, 0)

    def fill(k, carry):
        at_ref[k] = 0
        return carry

    lax.fori_loop(jnp.minimum(count, slots), slots, fill, 0)

    def start(i, carry):
        at = [at_ref[i * 8 + j] for j in range(8)]
        for j in range(8):
            pltpu.make_async_copy(table_ref.at[pl.ds(at[j], 1)], out_ref.at[pl.ds(i * 8 + j, 1)], sem).start()
        return carry

    lax.fori_loop(0, slots // 8, start, 0)
    pltpu.make_async_copy(out_ref, out_ref, sem).wait()


def join_kernel(first, even_ref, source_ref, slow_ref, *refs):
    blocks, out_ref, all_ref = refs[:-2], refs[-2], refs[-1]
    size, n = blocks[0].shape[0], out_ref.shape[0]

    @pl.when(even_ref[0] == 1)
    def _():
        for d, block in enumerate(blocks):
            all_ref[d * size:(d + 1) * size, :] = block[...]

        def copy(i, carry):
            at = [source_ref[first + i * 8 + j] for j in range(8)]
            out_ref[pl.ds(pl.multiple_of(i * 8, 8), 8), :] = jnp.concatenate([all_ref[pl.ds(a, 1), :] for a in at], 0)
            return carry

        lax.fori_loop(0, n // 8, copy, 0)

    @pl.when(even_ref[0] == 0)
    def _():
        pltpu.sync_copy(slow_ref.at[first:first + n], out_ref)


SMEM, VMEM, ANY = (pl.BlockSpec(memory_space=s) for s in (pltpu.SMEM, pltpu.VMEM, pl.ANY))


def f32(*shape):
    return jax.ShapeDtypeStruct(shape, jnp.float32)


GRANT = pltpu.CompilerParams(vmem_limit_bytes=20 * 2 ** 20)


def call(kernel, outs, specs, scratch, flops, *args):
    return pl.pallas_call(
        kernel,
        out_shape=outs,
        in_specs=specs,
        out_specs=(VMEM,) * len(outs) if isinstance(outs, tuple) else VMEM,
        scratch_shapes=scratch,
        cost_estimate=pl.CostEstimate(flops=flops, bytes_accessed=10 ** 6, transcendentals=0),
        compiler_params=GRANT,
    )(*args)


def partner(size, distance):
    return [(i, i ^ distance) for i in range(size)]


def tie(value, *after):
    return lax.optimization_barrier((value,) + after)[0]


def any_split(embeddings, offsets):
    n = lax.axis_size("row")
    inside = (offsets >= 0) & (offsets < embeddings.shape[0])
    rows = jnp.take(embeddings, jnp.clip(offsets, 0, embeddings.shape[0] - 1), axis=0)
    rows = jnp.where(inside[:, None], rows, 0.0).reshape(n, -1, embeddings.shape[1])
    share = jnp.sum(lax.all_to_all(rows, "row", 0, 0), 0)
    out = lax.all_to_all(jnp.broadcast_to(share[None], (n,) + share.shape), "row", 0, 0)
    return out.reshape(-1, embeddings.shape[1])


def steps(embeddings, selected):
    rows_here, width = embeddings.shape
    picks = selected.shape[0]
    row_size, col_size = lax.axis_size("row"), lax.axis_size("col")
    row, col = lax.axis_index("row"), lax.axis_index("col")
    core, half = col % 2, col // 2
    block = rows_here // col_size
    to_core = lambda v: lax.ppermute(v, "col", partner(col_size, 1))
    to_chip = lambda v: lax.ppermute(v, "col", partner(col_size, 2))
    to_row = lambda v, s: lax.ppermute(v, "row", partner(row_size, s))
    which_core = core.astype(jnp.int32)[None]

    spread = lambda share: 4.25 * math.sqrt(picks * share * (1 - share))
    slots = min(picks, math.ceil((picks / row_size + spread(1 / row_size)) / 8) * 8)
    least = lambda share: max(8, int((picks * share - spread(share)) / 8) * 8)
    own_rows = least(1 / row_size)
    near_rows = max(own_rows + 8, least(NEAR / row_size))
    sizes = (own_rows, near_rows - own_rows, picks - near_rows)

    other_embeddings = to_core(embeddings)

    rows = pl.pallas_call(
        pick_kernel,
        out_shape=f32(slots, width),
        in_specs=[SMEM, SMEM, ANY],
        out_specs=VMEM,
        scratch_shapes=[pltpu.SMEM((picks + 8,), jnp.int32), pltpu.SemaphoreType.DMA],
        compiler_params=GRANT,
    )(selected, (row * rows_here)[None], embeddings)
    far = [to_row(rows, s) for s in range(NEAR, row_size, NEAR)]
    around = [rows] + [to_row(rows, s) for s in range(1, NEAR)]

    picked = tie(selected, rows)
    shard = picked // rows_here
    number = jnp.arange(picks)
    before = number[None, :] < number[:, None]
    count = lambda mask: jnp.sum(mask, 1, dtype=jnp.int32)
    rank = count((shard[:, None] == shard[None, :]) & before)
    is_own = (shard == row) & (rank < own_rows)
    key = shard * picks + number
    around_here = (shard // NEAR == row // NEAR) & ~is_own
    place = own_rows + count(around_here[None, :] & (key[None, :] < key[:, None]))
    is_near = is_own | (around_here & (place < near_rows))
    place = jnp.where(is_own, rank, jnp.where(is_near, place, near_rows + count(before & ~is_near[None, :])))
    found = (shard ^ row) * slots + rank
    source = jnp.sum(jnp.where(place[None, :] == number[:, None], found[None, :], 0), 1)
    source = jnp.clip(source, 0, row_size * slots - 1)
    shards = jnp.arange(row_size)
    counts = count(shard[None, :] == shards[:, None])
    groups = count(shard[None, :] // NEAR == shards[:, None] // NEAR)
    even = jnp.all((counts >= own_rows) & (counts <= slots) & (groups >= near_rows))
    slow = lax.cond(even, lambda v: jnp.zeros((picks, width), jnp.float32),
                    lambda v: any_split(embeddings, v - row * rows_here), picked)
    even = even.astype(jnp.int32)[None]

    def join(first, n, blocks):
        return call(functools.partial(join_kernel, first), f32(n, width), [SMEM, SMEM, ANY] + [VMEM] * len(blocks),
                    [pltpu.VMEM((len(blocks) * slots, width), jnp.float32)], 10 ** 8,
                    even, source, slow, *blocks)

    away = prepare(2 * (1 - half) + core, block, embeddings, other_embeddings)
    own = join(0, own_rows, [rows])
    own_other = to_core(own)
    score_own = score(away, own, own_other)
    got_own = to_chip(score_own)

    near = join(own_rows, sizes[1], [tie(rows, score_own)] + around[1:])
    near_other = to_core(near)
    all_far = tie(jnp.concatenate(far, 0), near)
    beyond = [all_far] + [to_row(all_far, s) for s in range(1, NEAR)]
    beyond = [v[m * slots:(m + 1) * slots] for m in range(len(far)) for v in beyond]
    score_near = score(away[:2], near, near_other)
    got_near = to_chip(score_near)

    rest = join(near_rows, sizes[2], [tie(v, score_near) for v in around] + beyond)
    rest_other = to_core(rest)
    pieces = (own, own_other, near, near_other, rest, rest_other)
    half_pairs = len(pairs(picks // BLOCK)[0]) * BLOCK
    gram = call(gram_kernel, f32(half_pairs, BLOCK), [SMEM] + [VMEM] * 6, [pltpu.VMEM((picks, 2 * width), jnp.bfloat16)] * 3,
                4 * 10 ** 8, which_core, *pieces)
    gram_got = to_chip(gram)
    score_rest = score(away[:2], *lax.optimization_barrier((rest, rest_other, gram))[:2])
    got_rest = to_chip(score_rest)
    home = prepare(2 * half + core, block, tie(embeddings, score_rest), other_embeddings)
    score_home = score(home[:2], *pieces)

    gram = tie(gram + gram_got, score_home)
    inverse, logs = call(factor_kernel, (f32(picks, picks), f32(8, BLOCK)), [SMEM] + [VMEM] * 2,
                         [pltpu.VMEM((picks, 2 * picks), jnp.float32), pltpu.VMEM((BLOCK, 2 * BLOCK), jnp.float32)],
                         4 * 10 ** 9, which_core, gram, to_core(gram))

    devices = row_size * col_size
    gain, log_gain, total = call(functools.partial(gain_kernel, sizes), (f32(1, block), f32(1, block), f32(devices, BLOCK)), [VMEM] * 7,
                                 [pltpu.VMEM((picks, block), jnp.bfloat16)] * 2, 10 ** 8,
                                 inverse, logs, home[2], score_home, got_own, got_near, got_rest)
    totals = lax.all_to_all(total.reshape(devices, 1, BLOCK), ("row", "col"), 0, 0).reshape(devices, BLOCK)
    share, logdet = call(functools.partial(share_kernel, rows_here * row_size), (f32(1, block), f32(1, 1)), [VMEM] * 2, [],
                         10 ** 7, totals, gain)
    return (share.reshape(block), log_gain.reshape(block), logdet.reshape(()))


def solution(mesh):
    return jax.shard_map(
        steps,
        mesh=mesh,
        in_specs=(P("row", "col"), P()),
        out_specs=(P(("row", "col")), P(("row", "col")), P()),
        check_vma=False,
    )
```
